32 devices in a mesh: gx: 8 (over z, y), gy: 4 (over x, core).
Axes of the slice: x: 2, y: 2, z: 4, core: 2. Of those that a mesh axis runs over, the one named last changes fastest.
Arguments:
- goal_embed: bfloat16 [4096, 128], P(('gx', 'gy')), may hold values from -6 to 6
- goal_bins: int32 [4096], P(('gx', 'gy')), may hold values from 0 to 2047, as said below
- goal_weights: float32 [4096], P(('gx', 'gy')), may hold values from 0.1 to 10
Outputs:
- bin_mean: float32 [2048, 128], P(('gx', 'gy'))
- rarity: float32 [2048], P(('gx', 'gy'))
The draws below stay inside these ranges and needn't reach their ends.
Inputs may be any that keep to these rules, and one draw needn't show every extreme that they name: `goal_bins`: bin b belongs to owner b // 64, owners numbered in the order of gx then gy. Of the goals of one device, at most 8 fall in the bins of one owner; some owner receives exactly 8 goals from every device.
All inputs are finite; a program needn't handle non-finite values.
Results may differ from the reference program's by a relative error of at most 0.0029.
Values may be sent and summed in bfloat16 or wider, within the bound.
No kernel may reach another device: no remote copies, remote signals or barrier semaphores. Data moves between devices by JAX's collectives and lax.ppermute only.
A program may use at most 64 MiB of HBM per device.

```python
import math
import jax
import jax.numpy as jnp

E = 128
BINS_DEV = 64
G_DEV = 128
GOALS = 4096
BINS = 2048
N_GX = 8
N_GY = 4


def draw_goal_bins(key, part):
    devices = N_GX * N_GY
    capacity = max(2, 2 * G_DEV // devices)
    key_common = jax.random.fold_in(key, 11)
    key_blocks = jax.random.fold_in(key, 12)
    key_offset = jax.random.fold_in(key, 13)
    common = jax.random.randint(key_common, (), 0, devices).astype(jnp.int32)

    def one_block(block_key):
        key_slots = jax.random.fold_in(block_key, 1)
        key_order = jax.random.fold_in(block_key, 2)
        slots = jax.random.permutation(key_slots, (devices - 1) * capacity).astype(jnp.int32)
        others = slots[:G_DEV - capacity] // capacity
        others = others + (others >= common).astype(jnp.int32)
        owners = jnp.concatenate([jnp.zeros((capacity,), jnp.int32) + common, others.astype(jnp.int32)])
        return jax.random.permutation(key_order, owners).astype(jnp.int32)
    owners = jax.vmap(one_block)(jax.random.split(key_blocks, devices)).reshape(-1)
    offsets = jax.random.randint(key_offset, (G_DEV * devices,), 0, BINS_DEV).astype(jnp.int32)
    return (owners * BINS_DEV + offsets).astype(jnp.int32)


def steps_of(rng, extent, pieces, least, high):
    gain = 1.0
    for position, shards_of in pieces:
        draws = jax.random.uniform(jax.random.fold_in(jax.random.fold_in(rng, 6), position), (shards_of,), jnp.float32, least / len(pieces), high / len(pieces))
        gain = gain * jnp.repeat(jnp.exp(draws), extent[position] // shards_of).reshape((-1,) + (1,) * (len(extent) - 1 - position))
    return gain


def gaussian(stream_key, dims, spread, reach, cuts=(), kind=jnp.bfloat16):
    array = jax.random.normal(stream_key, dims, jnp.float32) * spread
    if len(cuts) > 0:
        array = steps_of(stream_key, dims, cuts, -0.22, 0.18) * array
    return jnp.clip(array, min=-reach, max=reach).astype(kind)


def setup_inputs(seed: int = 0) -> dict:
    streams_of = jax.random.split(jax.random.key(seed), 4)
    goal_embed = gaussian(streams_of[0], (GOALS, E), 1.0, 6.0, ((0, 32),))
    goal_bins = draw_goal_bins(jax.random.fold_in(streams_of[3], 71), 0)
    goal_weights = jnp.clip(jnp.exp(math.log(10.0) - 4.6051702 * jax.random.uniform(streams_of[2], (GOALS,), jnp.float32) ** steps_of(streams_of[2], (GOALS,), ((0, 32),), -0.2, 0.2)), 0.1, 10.0)
    return {"goal_embed": goal_embed, "goal_bins": goal_bins, "goal_weights": goal_weights}


def reference(goal_embed, goal_bins, goal_weights):
    scaled = (goal_weights[:, None] * goal_embed.astype(jnp.float32)).astype(jnp.bfloat16)
    bin_sums = jax.ops.segment_sum(scaled.astype(jnp.float32), goal_bins, num_segments=BINS)
    bin_mass = jax.ops.segment_sum(goal_weights, goal_bins, num_segments=BINS)
    total_mass = jnp.sum(goal_weights)
    bin_mean = bin_sums / (bin_mass[:, None] + 1.0)
    rarity = jnp.log(total_mass / BINS) - jnp.log(bin_mass + 1.0)
    return bin_mean, rarity
```

```python
import jax
import jax.numpy as jnp
from jax import lax
from jax.experimental import pallas as pl
from jax.experimental.pallas import tpu as pltpu
from jax.sharding import PartitionSpec as P

BINS_DEV = 64
LANES = 128
OFFSET = 3
SUM = 4


def pieces(x):
    hi = x.astype(jnp.bfloat16).astype(jnp.float32)
    rest = x - hi
    mid = rest.astype(jnp.bfloat16).astype(jnp.float32)
    return hi, mid, rest - mid


def pack(devices, capacity, embed_ref, bins_ref, weights_ref, out_ref):
    goals, width = embed_ref.shape
    bins = bins_ref[...]
    weights = weights_ref[...]
    owners = bins // BINS_DEV
    offsets = bins - owners * BINS_DEV
    owner_ids = lax.broadcasted_iota(jnp.int32, (devices, goals), 0)
    member = owner_ids == owners
    earlier = lax.broadcasted_iota(jnp.int32, (goals, goals), 0) < lax.broadcasted_iota(jnp.int32, (goals, goals), 1)
    before = jnp.dot(
        member.astype(jnp.bfloat16), earlier.astype(jnp.bfloat16), preferred_element_type=jnp.float32
    )
    places = jnp.sum(jnp.where(member, before, 0.0), axis=0, keepdims=True).astype(jnp.int32)
    slots = owners * capacity + places
    rows = lax.broadcasted_iota(jnp.int32, (devices * capacity, goals), 0)
    chosen = (rows == slots).astype(jnp.bfloat16)
    up = jnp.transpose(
        jnp.concatenate([weights, offsets.astype(jnp.float32), jnp.zeros((6, goals), jnp.float32)], axis=0)
    )
    weight = up[:, 0:1]
    offset = up[:, 1:2]
    scaled = (weight * embed_ref[...].astype(jnp.float32)).astype(jnp.bfloat16)
    lane = lax.broadcasted_iota(jnp.int32, (goals, LANES), 1)
    hi, mid, lo = pieces(weight)
    tag = jnp.where(lane == 0, hi, jnp.where(lane == 1, mid, jnp.where(lane == 2, lo, 0.0)))
    tag = jnp.where(lane == OFFSET, offset, tag).astype(jnp.bfloat16)
    out_ref[:, :width] = jnp.dot(chosen, scaled, preferred_element_type=jnp.float32).astype(jnp.bfloat16)
    tags = jnp.dot(chosen, tag, preferred_element_type=jnp.float32)
    hi, mid, lo = pieces(jnp.sum(weights, axis=1, keepdims=True))
    lane = lax.broadcasted_iota(jnp.int32, (1, LANES), 1)
    own = jnp.where(lane == SUM, hi, jnp.where(lane == SUM + 1, mid, jnp.where(lane == SUM + 2, lo, 0.0)))
    out_ref[:, width:] = (tags + own).astype(jnp.bfloat16)


def unpack(bins, capacity, in_ref, mean_ref, rarity_ref):
    width = mean_ref.shape[1]
    tags = in_ref[:, width:]
    offsets = tags[:, OFFSET : OFFSET + 1].astype(jnp.int32)
    labels = lax.broadcasted_iota(jnp.int32, (tags.shape[0], BINS_DEV), 1)
    selector = (offsets == labels).astype(jnp.bfloat16)
    over_rows = (((0,), (0,)), ((), ()))
    sums = lax.dot_general(selector, in_ref[:, :width], over_rows, preferred_element_type=jnp.float32)
    masses = lax.dot_general(selector, tags, over_rows, preferred_element_type=jnp.float32)
    mass = masses[:, 0:1] + masses[:, 1:2] + masses[:, 2:3] + 1.0
    mean_ref[...] = sums / mass
    totals = jnp.sum(tags.astype(jnp.float32), axis=0, keepdims=True)
    total = (totals[:, SUM : SUM + 1] + totals[:, SUM + 1 : SUM + 2] + totals[:, SUM + 2 : SUM + 3]) / capacity
    across = jnp.transpose(jnp.broadcast_to(mass, (BINS_DEV, LANES)))[0:1, :]
    rarity_ref[...] = jnp.log(total / bins) - jnp.log(across)


def shards(goal_embed, goal_bins, goal_weights):
    goals, width = goal_embed.shape
    devices = lax.axis_size("gx") * lax.axis_size("gy")
    capacity = max(2, 2 * goals // devices)
    outgoing = pl.pallas_call(
        lambda *refs: pack(devices, capacity, *refs),
        out_shape=jax.ShapeDtypeStruct((devices * capacity, width + LANES), jnp.bfloat16),
        name="pack",
    )(goal_embed, goal_bins.reshape(1, goals), goal_weights.reshape(1, goals))
    arrived = lax.all_to_all(
        outgoing.reshape(devices, capacity, width + LANES), ("gx", "gy"), split_axis=0, concat_axis=0, tiled=True
    )
    bin_mean, rarity = pl.pallas_call(
        lambda *refs: unpack(BINS_DEV * devices, capacity, *refs),
        out_shape=(
            jax.ShapeDtypeStruct((BINS_DEV, width), jnp.float32),
            jax.ShapeDtypeStruct((1, BINS_DEV), jnp.float32),
        ),
        name="unpack",
    )(arrived.reshape(devices * capacity, width + LANES))
    return bin_mean, rarity.reshape(BINS_DEV)


def solution(mesh):
    in_specs = (P(("gx", "gy"), None), P(("gx", "gy")), P(("gx", "gy")))
    out_specs = (P(("gx", "gy"), None), P(("gx", "gy")))
    return jax.shard_map(shards, mesh=mesh, in_specs=in_specs, out_specs=out_specs, check_vma=False)
```

```python
import jax
import jax.numpy as jnp
from jax import lax
from jax.experimental import pallas as pl
from jax.experimental.pallas import tpu as pltpu
from jax.sharding import PartitionSpec as P

BINS_DEV = 64
LANES = 128
VMEM_BYTES = 4 * 1024 * 1024
OFFSET = 3
SUM = 4


def pieces(x):
    hi = x.astype(jnp.bfloat16).astype(jnp.float32)
    rest = x - hi
    mid = rest.astype(jnp.bfloat16).astype(jnp.float32)
    return hi, mid, rest - mid


def pack(devices, capacity, embed_hbm, bins_hbm, weights_hbm, out_ref, embed_ref, bins_ref, weights_ref, arrivals):
    goals, width = embed_ref.shape
    copies = [
        pltpu.make_async_copy(source, target, arrivals.at[i])
        for i, (source, target) in enumerate(
            ((bins_hbm, bins_ref), (weights_hbm, weights_ref), (embed_hbm, embed_ref))
        )
    ]
    for copy in copies:
        copy.start()
    for copy in copies:
        copy.wait()
    bins = bins_ref[...]
    weights = weights_ref[...]
    owners = bins // BINS_DEV
    offsets = bins - owners * BINS_DEV
    owner_ids = lax.broadcasted_iota(jnp.int32, (devices, goals), 0)
    member = owner_ids == owners
    earlier = lax.broadcasted_iota(jnp.int32, (goals, goals), 0) < lax.broadcasted_iota(jnp.int32, (goals, goals), 1)
    before = jnp.dot(
        member.astype(jnp.bfloat16), earlier.astype(jnp.bfloat16), preferred_element_type=jnp.float32
    )
    places = jnp.sum(jnp.where(member, before, 0.0), axis=0, keepdims=True).astype(jnp.int32)
    slots = owners * capacity + places
    rows = lax.broadcasted_iota(jnp.int32, (devices * capacity, goals), 0)
    chosen = (rows == slots).astype(jnp.bfloat16)
    up = jnp.transpose(
        jnp.concatenate([weights, offsets.astype(jnp.float32), jnp.zeros((6, goals), jnp.float32)], axis=0)
    )
    weight = up[:, 0:1]
    offset = up[:, 1:2]
    scaled = (weight * embed_ref[...].astype(jnp.float32)).astype(jnp.bfloat16)
    lane = lax.broadcasted_iota(jnp.int32, (goals, LANES), 1)
    hi, mid, lo = pieces(weight)
    tag = jnp.where(lane == 0, hi, jnp.where(lane == 1, mid, jnp.where(lane == 2, lo, 0.0)))
    tag = jnp.where(lane == OFFSET, offset, tag).astype(jnp.bfloat16)
    out_ref[:, :width] = jnp.dot(chosen, scaled, preferred_element_type=jnp.float32).astype(jnp.bfloat16)
    tags = jnp.dot(chosen, tag, preferred_element_type=jnp.float32)
    hi, mid, lo = pieces(jnp.sum(weights, axis=1, keepdims=True))
    lane = lax.broadcasted_iota(jnp.int32, (1, LANES), 1)
    own = jnp.where(lane == SUM, hi, jnp.where(lane == SUM + 1, mid, jnp.where(lane == SUM + 2, lo, 0.0)))
    out_ref[:, width:] = (tags + own).astype(jnp.bfloat16)


def unpack(bins, capacity, in_ref, mean_ref, rarity_ref):
    width = mean_ref.shape[1]
    tags = in_ref[:, width:]
    offsets = tags[:, OFFSET : OFFSET + 1].astype(jnp.int32)
    labels = lax.broadcasted_iota(jnp.int32, (tags.shape[0], BINS_DEV), 1)
    selector = (offsets == labels).astype(jnp.bfloat16)
    over_rows = (((0,), (0,)), ((), ()))
    sums = lax.dot_general(selector, in_ref[:, :width], over_rows, preferred_element_type=jnp.float32)
    masses = lax.dot_general(selector, tags, over_rows, preferred_element_type=jnp.float32)
    mass = masses[:, 0:1] + masses[:, 1:2] + masses[:, 2:3] + 1.0
    mean_ref[...] = sums / mass
    totals = jnp.sum(tags.astype(jnp.float32), axis=0, keepdims=True)
    total = (totals[:, SUM : SUM + 1] + totals[:, SUM + 1 : SUM + 2] + totals[:, SUM + 2 : SUM + 3]) / capacity
    across = jnp.transpose(jnp.broadcast_to(mass, (BINS_DEV, LANES)))[0:1, :]
    rarity_ref[...] = jnp.log(total / bins) - jnp.log(across)


def shards(goal_embed, goal_bins, goal_weights):
    goals, width = goal_embed.shape
    devices = lax.axis_size("gx") * lax.axis_size("gy")
    capacity = max(2, 2 * goals // devices)
    inputs = (goal_embed, goal_bins.reshape(1, goals), goal_weights.reshape(1, goals))
    outgoing = pl.pallas_call(
        lambda *refs: pack(devices, capacity, *refs),
        out_shape=jax.ShapeDtypeStruct((devices * capacity, width + LANES), jnp.bfloat16),
        in_specs=[pl.BlockSpec(memory_space=pltpu.HBM)] * 3,
        scratch_shapes=[
            pltpu.VMEM((goals, width), goal_embed.dtype),
            pltpu.VMEM((1, goals), goal_bins.dtype),
            pltpu.VMEM((1, goals), goal_weights.dtype),
            pltpu.SemaphoreType.DMA((3,)),
        ],
        compiler_params=pltpu.CompilerParams(vmem_limit_bytes=VMEM_BYTES),
        name="pack",
    )(*(pltpu.with_memory_space_constraint(x, pltpu.HBM) for x in inputs))
    arrived = lax.all_to_all(
        outgoing.reshape(devices, capacity, width + LANES), ("gx", "gy"), split_axis=0, concat_axis=0, tiled=True
    )
    bin_mean, rarity = pl.pallas_call(
        lambda *refs: unpack(BINS_DEV * devices, capacity, *refs),
        out_shape=(
            jax.ShapeDtypeStruct((BINS_DEV, width), jnp.float32),
            jax.ShapeDtypeStruct((1, BINS_DEV), jnp.float32),
        ),
        compiler_params=pltpu.CompilerParams(vmem_limit_bytes=VMEM_BYTES),
        name="unpack",
    )(arrived.reshape(devices * capacity, width + LANES))
    return bin_mean, rarity.reshape(BINS_DEV)


def solution(mesh):
    in_specs = (P(("gx", "gy"), None), P(("gx", "gy")), P(("gx", "gy")))
    out_specs = (P(("gx", "gy"), None), P(("gx", "gy")))
    return jax.shard_map(shards, mesh=mesh, in_specs=in_specs, out_specs=out_specs, check_vma=False)
```

```python
import jax
import jax.numpy as jnp
from jax import lax
from jax.experimental import pallas as pl
from jax.experimental.pallas import tpu as pltpu
from jax.sharding import PartitionSpec as P

BINS_DEV = 64
LANES = 128
VMEM_BYTES = 4 * 1024 * 1024
OFFSET = 3
SUM = 4


def pieces(x):
    hi = x.astype(jnp.bfloat16).astype(jnp.float32)
    rest = x - hi
    mid = rest.astype(jnp.bfloat16).astype(jnp.float32)
    return hi, mid, rest - mid


def one_hot(mask):
    return jnp.where(mask, 1.0, 0.0).astype(jnp.bfloat16)


def iota(shape, dimension):
    return lax.broadcasted_iota(jnp.int32, shape, dimension)


def pack(devices, capacity, embed_hbm, bins_hbm, weights_hbm, out_ref, embed_ref, bins_ref, weights_ref, arrivals):
    goals = embed_ref.shape[0]
    copies = [
        pltpu.make_async_copy(source, target, arrivals.at[i])
        for i, (source, target) in enumerate(
            ((bins_hbm, bins_ref), (weights_hbm, weights_ref), (embed_hbm, embed_ref))
        )
    ]
    for copy in copies:
        copy.start()
    stride = capacity + 2
    rows = iota((devices * stride, goals), 0)
    for copy in copies:
        copy.wait()
    bins = bins_ref[...]
    weights = weights_ref[...]
    owners = bins // BINS_DEV
    offsets = (bins - owners * BINS_DEV).astype(jnp.float32)
    member = iota((devices, goals), 0) == owners
    earlier = iota((goals, goals), 0) < iota((goals, goals), 1)
    before = jnp.dot(one_hot(member), one_hot(earlier), preferred_element_type=jnp.float32)
    places = jnp.sum(jnp.where(member, before, 0.0), axis=0, keepdims=True).astype(jnp.int32)
    bases = owners * stride
    chosen = one_hot(rows == bases + places)
    up = jnp.transpose(jnp.concatenate([weights, jnp.zeros((7, goals), jnp.float32)], axis=0))
    scaled = (up[:, 0:1] * embed_ref[...].astype(jnp.float32)).astype(jnp.bfloat16)
    tagged = one_hot(rows == bases + capacity)
    hi, mid, lo = pieces(weights)
    lane = iota((LANES, goals), 0)
    tags = jnp.zeros((LANES, goals), jnp.float32)
    for field, value in enumerate((hi, mid, lo, offsets)):
        tags = jnp.where(lane == places + field * capacity, value, tags)
    lane = iota((LANES, devices), 0)
    own = jnp.zeros((LANES, devices), jnp.float32)
    for field, value in enumerate(pieces(jnp.sum(weights, axis=1, keepdims=True))):
        own = jnp.where(lane == SUM * capacity + field, value, own)
    every = one_hot(iota((devices * stride, devices), 0) == iota((devices * stride, devices), 1) * stride + capacity)
    across = (((1,), (1,)), ((), ()))
    out = jnp.dot(chosen, scaled, preferred_element_type=jnp.float32)
    out += lax.dot_general(tagged, tags.astype(jnp.bfloat16), across, preferred_element_type=jnp.float32)
    out += lax.dot_general(every, own.astype(jnp.bfloat16), across, preferred_element_type=jnp.float32)
    out_ref[...] = out.astype(jnp.bfloat16)


def unpack(devices, capacity, in_ref, mean_ref, rarity_ref):
    stride = capacity + 2
    slots = devices * stride
    arrived = in_ref[...]
    tag_rows = one_hot(iota((devices, slots), 1) == iota((devices, slots), 0) * stride + capacity)
    tags = jnp.dot(tag_rows, arrived, preferred_element_type=jnp.float32)
    slot = iota((LANES, slots), 1)
    place = slot - ((slot.astype(jnp.float32) + 0.5) * (1.0 / stride)).astype(jnp.int32) * stride
    lane = iota((LANES, slots), 0)
    pick = one_hot(lane == place + OFFSET * capacity)
    gather = one_hot((lane == place) | (lane == place + capacity) | (lane == place + 2 * capacity))
    first = iota((devices, slots), 1) - iota((devices, slots), 0) * stride
    here = (first >= 0) & (first < capacity)
    tags = tags.astype(jnp.bfloat16)
    offsets = jnp.dot(tags, pick, preferred_element_type=jnp.float32)
    weights = jnp.dot(tags, gather, preferred_element_type=jnp.float32)
    offsets = jnp.sum(jnp.where(here, offsets + 1.0, 0.0), axis=0, keepdims=True)
    weights = jnp.sum(jnp.where(here, weights, 0.0), axis=0, keepdims=True)
    selector = iota((BINS_DEV, slots), 0) + 1 == offsets.astype(jnp.int32)
    sums = jnp.dot(one_hot(selector), arrived, preferred_element_type=jnp.float32)
    mass = jnp.sum(jnp.where(selector, weights, 0.0), axis=1, keepdims=True) + 1.0
    mean_ref[...] = sums / mass
    totals = jnp.sum(tags.astype(jnp.float32), axis=0, keepdims=True)
    lane = iota(totals.shape, 1)
    own = (lane >= SUM * capacity) & (lane < SUM * capacity + 3)
    total = jnp.sum(jnp.where(own, totals, 0.0), axis=1, keepdims=True)
    across = jnp.transpose(jnp.broadcast_to(mass, (BINS_DEV, LANES)))[0:1, :]
    rarity_ref[...] = jnp.log(total / (BINS_DEV * devices)) - jnp.log(across)


def shards(goal_embed, goal_bins, goal_weights):
    goals, width = goal_embed.shape
    devices = lax.axis_size("gx") * lax.axis_size("gy")
    capacity = max(2, 2 * goals // devices)
    capacity += capacity % 2
    stride = capacity + 2
    inputs = (goal_embed, goal_bins.reshape(1, goals), goal_weights.reshape(1, goals))
    outgoing = pl.pallas_call(
        lambda *refs: pack(devices, capacity, *refs),
        out_shape=jax.ShapeDtypeStruct((devices * stride, width), jnp.bfloat16),
        in_specs=[pl.BlockSpec(memory_space=pltpu.HBM)] * 3,
        scratch_shapes=[
            pltpu.VMEM((goals, width), goal_embed.dtype),
            pltpu.VMEM((1, goals), goal_bins.dtype),
            pltpu.VMEM((1, goals), goal_weights.dtype),
            pltpu.SemaphoreType.DMA((3,)),
        ],
        compiler_params=pltpu.CompilerParams(vmem_limit_bytes=VMEM_BYTES),
        name="pack",
    )(*(pltpu.with_memory_space_constraint(x, pltpu.HBM) for x in inputs))
    arrived = lax.all_to_all(
        outgoing.reshape(devices, stride // 2, 2, width), ("gx", "gy"), split_axis=0, concat_axis=0, tiled=True
    )
    bin_mean, rarity = pl.pallas_call(
        lambda *refs: unpack(devices, capacity, *refs),
        out_shape=(
            jax.ShapeDtypeStruct((BINS_DEV, width), jnp.float32),
            jax.ShapeDtypeStruct((1, BINS_DEV), jnp.float32),
        ),
        compiler_params=pltpu.CompilerParams(vmem_limit_bytes=VMEM_BYTES),
        name="unpack",
    )(arrived.reshape(devices * stride, width))
    return bin_mean, rarity.reshape(BINS_DEV)


def solution(mesh):
    in_specs = (P(("gx", "gy"), None), P(("gx", "gy")), P(("gx", "gy")))
    out_specs = (P(("gx", "gy"), None), P(("gx", "gy")))
    return jax.shard_map(shards, mesh=mesh, in_specs=in_specs, out_specs=out_specs, check_vma=False)
```

```python
import jax
import jax.numpy as jnp
from jax import lax
from jax.experimental import pallas as pl
from jax.experimental.pallas import tpu as pltpu
from jax.sharding import PartitionSpec as P

BINS_DEV = 64
LANES = 128
VMEM_BYTES = 4 * 1024 * 1024
FIELD = LANES // 4


def pieces(x):
    hi = x.astype(jnp.bfloat16).astype(jnp.float32)
    rest = x - hi
    mid = rest.astype(jnp.bfloat16).astype(jnp.float32)
    return hi, mid, rest - mid


def one_hot(mask):
    return jnp.where(mask, 1.0, 0.0).astype(jnp.bfloat16)


def iota(shape, dimension):
    return lax.broadcasted_iota(jnp.int32, shape, dimension)


def pack(devices, capacity, embed_hbm, bins_hbm, weights_hbm, out_ref, embed_ref, bins_ref, weights_ref, stage_ref, arrivals):
    goals = embed_ref.shape[0]
    copies = [
        pltpu.make_async_copy(source, target, arrivals.at[i])
        for i, (source, target) in enumerate(
            ((bins_hbm, bins_ref), (weights_hbm, weights_ref), (embed_hbm, embed_ref))
        )
    ]
    for copy in copies:
        copy.start()
    stride = capacity + 2
    rows = iota((devices * stride, goals), 0)
    for copy in copies:
        copy.wait()
    bins = bins_ref[...]
    weights = weights_ref[...]
    owners = bins // BINS_DEV
    offsets = (bins - owners * BINS_DEV).astype(jnp.float32)
    member = iota((devices, goals), 0) == owners
    earlier = iota((goals, goals), 0) < iota((goals, goals), 1)
    before = jnp.dot(one_hot(member), one_hot(earlier), preferred_element_type=jnp.float32)
    places = jnp.sum(jnp.where(member, before, 0.0), axis=0, keepdims=True).astype(jnp.int32)
    chosen = one_hot(rows == owners * stride + places)
    up = jnp.transpose(jnp.concatenate([weights, jnp.zeros((7, goals), jnp.float32)], axis=0))
    scaled = (up[:, 0:1] * embed_ref[...].astype(jnp.float32)).astype(jnp.bfloat16)
    me = lax.axis_index("gx") * lax.axis_size("gy") + lax.axis_index("gy")
    lane = lax.rem(iota((LANES, goals), 0) + (LANES - lax.rem(me * stride, LANES)), LANES)
    tags = jnp.zeros((LANES, goals), jnp.float32)
    for field, value in enumerate((offsets, *pieces(weights))):
        tags = jnp.where(lane == places + field * FIELD, value, tags)
    across = (((1,), (1,)), ((), ()))
    tags = lax.dot_general(
        one_hot(member), tags.astype(jnp.bfloat16), across, preferred_element_type=jnp.float32
    )
    lane = lax.rem(iota(tags.shape, 1) + (LANES - lax.rem(me * stride, LANES)), LANES)
    for i, piece in enumerate(pieces(jnp.sum(weights, axis=1, keepdims=True))):
        tags = jnp.where(lane == capacity + i, piece, tags)
    stage_ref[...] = jnp.dot(chosen, scaled, preferred_element_type=jnp.float32)
    stage_ref[pl.ds(capacity, devices, stride=stride), :] = tags
    out_ref[...] = stage_ref[...].astype(jnp.bfloat16)


def unpack(devices, capacity, in_ref, mean_ref, rarity_ref, stage_ref):
    stride = capacity + 2
    slots = devices * stride
    stage_ref[...] = in_ref[...].astype(jnp.float32)
    tags = stage_ref[pl.ds(capacity, devices, stride=stride), :]
    fields = [tags, *(pltpu.roll(tags, LANES - field * FIELD, 1) for field in range(1, 4))]
    tiles = pl.cdiv(slots, LANES)
    place = iota((devices, tiles * LANES), 1) - iota((devices, tiles * LANES), 0) * stride
    here = (place >= 0) & (place < capacity)

    def spread(x):
        return jnp.sum(jnp.where(here, jnp.concatenate([x] * tiles, axis=1), 0.0), axis=0, keepdims=True)

    offsets = spread(fields[0] + 1.0)
    weights = spread(fields[1] + fields[2] + fields[3])
    selector = iota((BINS_DEV, tiles * LANES), 0) + 1 == offsets.astype(jnp.int32)
    chosen = one_hot(selector)
    sums = jnp.dot(chosen[:, :slots], in_ref[...], preferred_element_type=jnp.float32)
    mass = jnp.sum(jnp.where(selector, weights, 0.0), axis=1, keepdims=True) + 1.0
    mean_ref[...] = sums / mass
    turned = LANES - lax.rem(iota(tags.shape, 0) * stride, LANES)
    lane = lax.rem(iota(tags.shape, 1) + turned, LANES)
    own = (lane >= capacity) & (lane < capacity + 3)
    total = jnp.sum(jnp.sum(jnp.where(own, tags, 0.0), axis=0, keepdims=True), axis=1, keepdims=True)
    parts = jnp.concatenate([*pieces(weights), jnp.zeros((5, tiles * LANES), jnp.float32)], axis=0)
    across = (((1,), (1,)), ((), ()))
    masses = lax.dot_general(parts.astype(jnp.bfloat16), chosen, across, preferred_element_type=jnp.float32)
    masses = jnp.sum(masses, axis=0, keepdims=True) + 1.0
    rarity_ref[...] = jnp.log(total / (BINS_DEV * devices)) - jnp.log(masses)


def shards(goal_embed, goal_bins, goal_weights):
    goals, width = goal_embed.shape
    devices = lax.axis_size("gx") * lax.axis_size("gy")
    capacity = max(2, 2 * goals // devices)
    capacity += capacity % 2
    stride = capacity + 2
    inputs = (goal_embed, goal_bins.reshape(1, goals), goal_weights.reshape(1, goals))
    outgoing = pl.pallas_call(
        lambda *refs: pack(devices, capacity, *refs),
        out_shape=jax.ShapeDtypeStruct((devices * stride, width), jnp.bfloat16),
        in_specs=[pl.BlockSpec(memory_space=pltpu.HBM)] * 3,
        scratch_shapes=[
            pltpu.VMEM((goals, width), goal_embed.dtype),
            pltpu.VMEM((1, goals), goal_bins.dtype),
            pltpu.VMEM((1, goals), goal_weights.dtype),
            pltpu.VMEM((devices * stride, width), jnp.float32),
            pltpu.SemaphoreType.DMA((3,)),
        ],
        compiler_params=pltpu.CompilerParams(vmem_limit_bytes=VMEM_BYTES),
        name="pack",
    )(*(pltpu.with_memory_space_constraint(x, pltpu.HBM) for x in inputs))
    arrived = lax.all_to_all(
        outgoing.reshape(devices, stride // 2, 2, width), ("gx", "gy"), split_axis=0, concat_axis=0, tiled=True
    )
    bin_mean, rarity = pl.pallas_call(
        lambda *refs: unpack(devices, capacity, *refs),
        out_shape=(
            jax.ShapeDtypeStruct((BINS_DEV, width), jnp.float32),
            jax.ShapeDtypeStruct((1, BINS_DEV), jnp.float32),
        ),
        scratch_shapes=[pltpu.VMEM((devices * stride, width), jnp.float32)],
        compiler_params=pltpu.CompilerParams(vmem_limit_bytes=VMEM_BYTES),
        name="unpack",
    )(arrived.reshape(devices * stride, width))
    return bin_mean, rarity.reshape(BINS_DEV)


def solution(mesh):
    in_specs = (P(("gx", "gy"), None), P(("gx", "gy")), P(("gx", "gy")))
    out_specs = (P(("gx", "gy"), None), P(("gx", "gy")))
    return jax.shard_map(shards, mesh=mesh, in_specs=in_specs, out_specs=out_specs, check_vma=False)
```

```python
import jax
import jax.numpy as jnp
from jax import lax
from jax.experimental import pallas as pl
from jax.experimental.pallas import tpu as pltpu
from jax.sharding import PartitionSpec as P

BINS_DEV = 64
LANES = 128
VMEM_BYTES = 4 * 1024 * 1024
FIELD = LANES // 4


def pieces(x):
    hi = x.astype(jnp.bfloat16).astype(jnp.float32)
    rest = x - hi
    mid = rest.astype(jnp.bfloat16).astype(jnp.float32)
    return hi, mid, rest - mid


def one_hot(mask):
    return jnp.where(mask, 1.0, 0.0).astype(jnp.bfloat16)


def quotient(x, n):
    return x >> (n.bit_length() - 1) if n & (n - 1) == 0 else lax.div(x, n)


def iota(shape, dimension):
    return lax.broadcasted_iota(jnp.int32, shape, dimension)


def pack(capacity, embed_hbm, bins_hbm, weights_hbm, out_ref, embed_ref, bins_ref, weights_ref, stage_ref, arrivals):
    goals = embed_ref.shape[0]
    across, along = lax.axis_size("gx"), lax.axis_size("gy")
    devices = across * along
    copies = [
        pltpu.make_async_copy(source, target, arrivals.at[i])
        for i, (source, target) in enumerate(
            ((bins_hbm, bins_ref), (weights_hbm, weights_ref), (embed_hbm, embed_ref))
        )
    ]
    for copy in copies:
        copy.start()
    stride = capacity + 2
    rows = iota((devices * stride, goals), 0)
    for copy in copies:
        copy.wait()
    bins = bins_ref[...]
    weights = weights_ref[...]
    owners = quotient(bins, BINS_DEV)
    offsets = (bins - owners * BINS_DEV).astype(jnp.float32)
    major = quotient(owners, along)
    owners = (owners - major * along) * across + major
    member = iota((devices, goals), 0) == owners
    earlier = iota((goals, goals), 0) < iota((goals, goals), 1)
    before = jnp.dot(one_hot(member), one_hot(earlier), preferred_element_type=jnp.float32)
    places = jnp.sum(jnp.where(member, before, 0.0), axis=0, keepdims=True).astype(jnp.int32)
    chosen = one_hot(rows == owners * stride + places)
    up = jnp.transpose(jnp.concatenate([weights, jnp.zeros((7, goals), jnp.float32)], axis=0))
    scaled = (up[:, 0:1] * embed_ref[...].astype(jnp.float32)).astype(jnp.bfloat16)
    me = lax.axis_index("gy") * across + lax.axis_index("gx")
    lane = lax.rem(iota((LANES, goals), 0) + (LANES - lax.rem(me * stride, LANES)), LANES)
    tags = jnp.zeros((LANES, goals), jnp.float32)
    for field, value in enumerate((offsets, *pieces(weights))):
        tags = jnp.where(lane == places + field * FIELD, value, tags)
    over_lanes = (((1,), (1,)), ((), ()))
    tags = lax.dot_general(
        one_hot(member), tags.astype(jnp.bfloat16), over_lanes, preferred_element_type=jnp.float32
    )
    lane = lax.rem(iota(tags.shape, 1) + (LANES - lax.rem(me * stride, LANES)), LANES)
    for i, piece in enumerate(pieces(jnp.sum(weights, axis=1, keepdims=True))):
        tags = jnp.where(lane == capacity + i, piece, tags)
    stage_ref[...] = jnp.dot(chosen, scaled, preferred_element_type=jnp.float32)
    stage_ref[pl.ds(capacity, devices, stride=stride), :] = tags
    out_ref[...] = stage_ref[...].astype(jnp.bfloat16)


def unpack(devices, capacity, in_ref, mean_ref, rarity_ref, stage_ref):
    stride = capacity + 2
    slots = devices * stride
    stage_ref[...] = in_ref[...].astype(jnp.float32)
    tags = stage_ref[pl.ds(capacity, devices, stride=stride), :]
    fields = [tags, *(pltpu.roll(tags, LANES - field * FIELD, 1) for field in range(1, 4))]
    tiles = pl.cdiv(slots, LANES)
    place = iota((devices, tiles * LANES), 1) - iota((devices, tiles * LANES), 0) * stride
    here = (place >= 0) & (place < capacity)

    def spread(x):
        return jnp.sum(jnp.where(here, jnp.concatenate([x] * tiles, axis=1), 0.0), axis=0, keepdims=True)

    offsets = spread(fields[0] + 1.0)
    weights = spread(fields[1] + fields[2] + fields[3])
    selector = iota((BINS_DEV, tiles * LANES), 0) + 1 == offsets.astype(jnp.int32)
    chosen = one_hot(selector)
    sums = jnp.dot(chosen[:, :slots], in_ref[...], preferred_element_type=jnp.float32)
    mass = jnp.sum(jnp.where(selector, weights, 0.0), axis=1, keepdims=True) + 1.0
    mean_ref[...] = sums / mass
    turned = LANES - lax.rem(iota(tags.shape, 0) * stride, LANES)
    lane = lax.rem(iota(tags.shape, 1) + turned, LANES)
    own = (lane >= capacity) & (lane < capacity + 3)
    total = jnp.sum(jnp.sum(jnp.where(own, tags, 0.0), axis=0, keepdims=True), axis=1, keepdims=True)
    parts = jnp.concatenate([*pieces(weights), jnp.zeros((5, tiles * LANES), jnp.float32)], axis=0)
    over_lanes = (((1,), (1,)), ((), ()))
    masses = lax.dot_general(parts.astype(jnp.bfloat16), chosen, over_lanes, preferred_element_type=jnp.float32)
    masses = jnp.sum(masses, axis=0, keepdims=True) + 1.0
    rarity_ref[...] = jnp.log(total / (BINS_DEV * devices)) - jnp.log(masses)


def shards(goal_embed, goal_bins, goal_weights):
    goals, width = goal_embed.shape
    devices = lax.axis_size("gx") * lax.axis_size("gy")
    capacity = max(2, 2 * goals // devices)
    capacity += capacity % 2
    stride = capacity + 2
    inputs = (goal_embed, goal_bins.reshape(1, goals), goal_weights.reshape(1, goals))
    outgoing = pl.pallas_call(
        lambda *refs: pack(capacity, *refs),
        out_shape=jax.ShapeDtypeStruct((devices * stride, width), jnp.bfloat16),
        in_specs=[pl.BlockSpec(memory_space=pltpu.HBM)] * 3,
        scratch_shapes=[
            pltpu.VMEM((goals, width), goal_embed.dtype),
            pltpu.VMEM((1, goals), goal_bins.dtype),
            pltpu.VMEM((1, goals), goal_weights.dtype),
            pltpu.VMEM((devices * stride, width), jnp.float32),
            pltpu.SemaphoreType.DMA((3,)),
        ],
        compiler_params=pltpu.CompilerParams(vmem_limit_bytes=VMEM_BYTES),
        name="pack",
    )(*(pltpu.with_memory_space_constraint(x, pltpu.HBM) for x in inputs))
    arrived = lax.all_to_all(
        outgoing.reshape(devices, stride // 2, 2, width), ("gy", "gx"), split_axis=0, concat_axis=0, tiled=True
    )
    bin_mean, rarity = pl.pallas_call(
        lambda *refs: unpack(devices, capacity, *refs),
        out_shape=(
            jax.ShapeDtypeStruct((BINS_DEV, width), jnp.float32),
            jax.ShapeDtypeStruct((1, BINS_DEV), jnp.float32),
        ),
        scratch_shapes=[pltpu.VMEM((devices * stride, width), jnp.float32)],
        compiler_params=pltpu.CompilerParams(vmem_limit_bytes=VMEM_BYTES),
        name="unpack",
    )(arrived.reshape(devices * stride, width))
    return bin_mean, rarity.reshape(BINS_DEV)


def solution(mesh):
    in_specs = (P(("gx", "gy"), None), P(("gx", "gy")), P(("gx", "gy")))
    out_specs = (P(("gx", "gy"), None), P(("gx", "gy")))
    return jax.shard_map(shards, mesh=mesh, in_specs=in_specs, out_specs=out_specs, check_vma=False)
```

```python
import jax
import jax.numpy as jnp
from jax import lax
from jax.experimental import pallas as pl
from jax.experimental.pallas import tpu as pltpu
from jax.sharding import PartitionSpec as P

BINS_DEV = 64
LANES = 128
VMEM_BYTES = 4 * 1024 * 1024
FIELD = LANES // 4


def pieces(x):
    hi = x.astype(jnp.bfloat16).astype(jnp.float32)
    rest = x - hi
    mid = rest.astype(jnp.bfloat16).astype(jnp.float32)
    return hi, mid, rest - mid


def one_hot(mask):
    return jnp.where(mask, 1.0, 0.0).astype(jnp.bfloat16)


def quotient(x, n):
    return x >> (n.bit_length() - 1) if n & (n - 1) == 0 else lax.div(x, n)


def iota(shape, dimension):
    return lax.broadcasted_iota(jnp.int32, shape, dimension)


def pack(capacity, embed_hbm, bins_hbm, weights_hbm, out_ref, embed_ref, bins_ref, weights_ref, stage_ref, arrivals):
    goals = embed_ref.shape[0]
    across, along = lax.axis_size("gx"), lax.axis_size("gy")
    devices = across * along
    copies = [
        pltpu.make_async_copy(source, target, arrivals.at[i])
        for i, (source, target) in enumerate(
            ((bins_hbm, bins_ref), (weights_hbm, weights_ref), (embed_hbm, embed_ref))
        )
    ]
    for copy in copies:
        copy.start()
    stride = capacity + 2
    rows = iota((devices * stride, goals), 0)
    for copy in copies[:2]:
        copy.wait()
    bins = bins_ref[...]
    weights = weights_ref[...]
    owners = quotient(bins, BINS_DEV)
    offsets = (bins - owners * BINS_DEV).astype(jnp.float32)
    major = quotient(owners, along)
    owners = (owners - major * along) * across + major
    member = iota((devices, goals), 0) == owners
    earlier = iota((goals, goals), 0) < iota((goals, goals), 1)
    before = jnp.dot(one_hot(member), one_hot(earlier), preferred_element_type=jnp.float32)
    places = jnp.sum(jnp.where(member, before, 0.0), axis=0, keepdims=True).astype(jnp.int32)
    chosen = one_hot(rows == owners * stride + places)
    up = jnp.transpose(jnp.concatenate([weights, jnp.zeros((7, goals), jnp.float32)], axis=0))
    copies[2].wait()
    scaled = (up[:, 0:1] * embed_ref[...].astype(jnp.float32)).astype(jnp.bfloat16)
    me = lax.axis_index("gy") * across + lax.axis_index("gx")
    tall = pl.cdiv(capacity, 8) * 8
    place = iota((tall, goals), 0) == places
    blank = jnp.zeros((FIELD - tall, goals), jnp.float32)
    tags = []
    for value in (offsets, *pieces(weights)):
        tags += [jnp.where(place, value, 0.0), blank]
    tags = jnp.concatenate(tags, axis=0)
    over_lanes = (((1,), (1,)), ((), ()))
    tags = lax.dot_general(
        one_hot(member), tags.astype(jnp.bfloat16), over_lanes, preferred_element_type=jnp.float32
    )
    lane = iota(tags.shape, 1)
    for i, piece in enumerate(pieces(jnp.sum(weights, axis=1, keepdims=True))):
        tags = jnp.where(lane == capacity + i, piece, tags)
    stage_ref[...] = jnp.dot(chosen, scaled, preferred_element_type=jnp.float32)
    tags = pltpu.roll(tags, (me * stride) & (LANES - 1), 1)
    stage_ref[pl.ds(capacity, devices, stride=stride), :] = tags
    out_ref[...] = stage_ref[...].astype(jnp.bfloat16)


def unpack(devices, capacity, in_ref, mean_ref, rarity_ref, stage_ref):
    stride = capacity + 2
    slots = devices * stride
    stage_ref[...] = in_ref[...].astype(jnp.float32)
    tags = stage_ref[pl.ds(capacity, devices, stride=stride), :]
    fields = [tags, *(pltpu.roll(tags, LANES - field * FIELD, 1) for field in range(1, 4))]
    tiles = pl.cdiv(slots, LANES)
    place = iota((devices, tiles * LANES), 1) - iota((devices, tiles * LANES), 0) * stride
    here = (place >= 0) & (place < capacity)

    def spread(x):
        return jnp.sum(jnp.where(here, jnp.concatenate([x] * tiles, axis=1), 0.0), axis=0, keepdims=True)

    offsets = spread(fields[0] + 1.0)
    weights = spread(fields[1] + fields[2] + fields[3])
    selector = iota((BINS_DEV, tiles * LANES), 0) + 1 == offsets.astype(jnp.int32)
    chosen = one_hot(selector)
    sums = jnp.dot(chosen[:, :slots], in_ref[...], preferred_element_type=jnp.float32)
    mass = jnp.sum(jnp.where(selector, weights, 0.0), axis=1, keepdims=True) + 1.0
    mean_ref[...] = sums / mass
    lane = (iota(tags.shape, 1) - iota(tags.shape, 0) * stride) & (LANES - 1)
    own = (lane >= capacity) & (lane < capacity + 3)
    total = jnp.sum(jnp.sum(jnp.where(own, tags, 0.0), axis=0, keepdims=True), axis=1, keepdims=True)
    parts = jnp.concatenate([*pieces(weights), jnp.zeros((5, tiles * LANES), jnp.float32)], axis=0)
    over_lanes = (((1,), (1,)), ((), ()))
    masses = lax.dot_general(parts.astype(jnp.bfloat16), chosen, over_lanes, preferred_element_type=jnp.float32)
    masses = jnp.sum(masses, axis=0, keepdims=True) + 1.0
    rarity_ref[...] = jnp.log(total / (BINS_DEV * devices)) - jnp.log(masses)


def shards(goal_embed, goal_bins, goal_weights):
    goals, width = goal_embed.shape
    devices = lax.axis_size("gx") * lax.axis_size("gy")
    capacity = max(2, 2 * goals // devices)
    capacity += capacity % 2
    stride = capacity + 2
    inputs = (goal_embed, goal_bins.reshape(1, goals), goal_weights.reshape(1, goals))
    outgoing = pl.pallas_call(
        lambda *refs: pack(capacity, *refs),
        out_shape=jax.ShapeDtypeStruct((devices * stride, width), jnp.bfloat16),
        in_specs=[pl.BlockSpec(memory_space=pltpu.HBM)] * 3,
        scratch_shapes=[
            pltpu.VMEM((goals, width), goal_embed.dtype),
            pltpu.VMEM((1, goals), goal_bins.dtype),
            pltpu.VMEM((1, goals), goal_weights.dtype),
            pltpu.VMEM((devices * stride, width), jnp.float32),
            pltpu.SemaphoreType.DMA((3,)),
        ],
        compiler_params=pltpu.CompilerParams(vmem_limit_bytes=VMEM_BYTES),
        name="pack",
    )(*(pltpu.with_memory_space_constraint(x, pltpu.HBM) for x in inputs))
    arrived = lax.all_to_all(
        outgoing.reshape(devices, stride // 2, 2, width), ("gy", "gx"), split_axis=0, concat_axis=0, tiled=True
    )
    bin_mean, rarity = pl.pallas_call(
        lambda *refs: unpack(devices, capacity, *refs),
        out_shape=(
            jax.ShapeDtypeStruct((BINS_DEV, width), jnp.float32),
            jax.ShapeDtypeStruct((1, BINS_DEV), jnp.float32),
        ),
        scratch_shapes=[pltpu.VMEM((devices * stride, width), jnp.float32)],
        compiler_params=pltpu.CompilerParams(vmem_limit_bytes=VMEM_BYTES),
        name="unpack",
    )(arrived.reshape(devices * stride, width))
    return bin_mean, rarity.reshape(BINS_DEV)


def solution(mesh):
    in_specs = (P(("gx", "gy"), None), P(("gx", "gy")), P(("gx", "gy")))
    out_specs = (P(("gx", "gy"), None), P(("gx", "gy")))
    return jax.shard_map(shards, mesh=mesh, in_specs=in_specs, out_specs=out_specs, check_vma=False)
```

```python
import jax
import jax.numpy as jnp
from jax import lax
from jax.experimental import pallas as pl
from jax.experimental.pallas import tpu as pltpu
from jax.sharding import PartitionSpec as P

BINS_DEV = 64
LANES = 128
VMEM_BYTES = 4 * 1024 * 1024
FIELD = LANES // 4


def pieces(x):
    hi = x.astype(jnp.bfloat16).astype(jnp.float32)
    rest = x - hi
    mid = rest.astype(jnp.bfloat16).astype(jnp.float32)
    return hi, mid, rest - mid


def one_hot(mask):
    return jnp.where(mask, 1.0, 0.0).astype(jnp.bfloat16)


def quotient(x, n):
    return x >> (n.bit_length() - 1) if n & (n - 1) == 0 else lax.div(x, n)


def iota(shape, dimension):
    return lax.broadcasted_iota(jnp.int32, shape, dimension)


def pack(capacity, embed_hbm, bins_hbm, weights_hbm, out_ref, embed_ref, bins_ref, weights_ref, stage_ref, arrivals):
    goals = embed_ref.shape[0]
    across, along = lax.axis_size("gx"), lax.axis_size("gy")
    devices = across * along
    copies = [
        pltpu.make_async_copy(source, target, arrivals.at[i])
        for i, (source, target) in enumerate(
            ((bins_hbm, bins_ref), (weights_hbm, weights_ref), (embed_hbm, embed_ref))
        )
    ]
    for copy in copies:
        copy.start()
    stride = capacity + 2
    rows = iota((devices * stride, goals), 0)
    for copy in copies[:2]:
        copy.wait()
    bins = bins_ref[...]
    weights = weights_ref[...]
    owners = quotient(bins, BINS_DEV)
    offsets = (bins - owners * BINS_DEV).astype(jnp.float32)
    major = quotient(owners, along)
    owners = (owners - major * along) * across + major
    member = iota((devices, goals), 0) == owners
    earlier = iota((goals, goals), 0) < iota((goals, goals), 1)
    before = jnp.dot(one_hot(member), one_hot(earlier), preferred_element_type=jnp.float32)
    places = jnp.sum(jnp.where(member, before, 0.0), axis=0, keepdims=True).astype(jnp.int32)
    chosen = one_hot(rows == owners * stride + places)
    column = jnp.transpose(jnp.broadcast_to(weights, (embed_ref.shape[1], goals)))
    copies[2].wait()
    scaled = (column * embed_ref[...].astype(jnp.float32)).astype(jnp.bfloat16)
    me = lax.axis_index("gy") * across + lax.axis_index("gx")
    tall = pl.cdiv(capacity, 8) * 8
    place = iota((tall, goals), 0) == places
    blank = jnp.zeros((FIELD - tall, goals), jnp.float32)
    tags = []
    for value in (offsets, *pieces(weights)):
        tags += [jnp.where(place, value, 0.0), blank]
    tags = jnp.concatenate(tags, axis=0)
    over_lanes = (((1,), (1,)), ((), ()))
    tags = lax.dot_general(
        one_hot(member), tags.astype(jnp.bfloat16), over_lanes, preferred_element_type=jnp.float32
    )
    lane = iota(tags.shape, 1)
    for i, piece in enumerate(pieces(jnp.sum(weights, axis=1, keepdims=True))):
        tags = jnp.where(lane == capacity + i, piece, tags)
    stage_ref[...] = jnp.dot(chosen, scaled, preferred_element_type=jnp.float32)
    tags = pltpu.roll(tags, (me * stride) & (LANES - 1), 1)
    stage_ref[pl.ds(capacity, devices, stride=stride), :] = tags
    out_ref[...] = stage_ref[...].astype(jnp.bfloat16)


def unpack(devices, capacity, in_ref, mean_ref, rarity_ref, stage_ref):
    stride = capacity + 2
    slots = devices * stride
    stage_ref[...] = in_ref[...].astype(jnp.float32)
    tags = stage_ref[pl.ds(capacity, devices, stride=stride), :]
    fields = [tags, *(pltpu.roll(tags, LANES - field * FIELD, 1) for field in range(1, 4))]
    tiles = pl.cdiv(slots, LANES)
    place = iota((devices, tiles * LANES), 1) - iota((devices, tiles * LANES), 0) * stride
    here = (place >= 0) & (place < capacity)

    def spread(x):
        return jnp.sum(jnp.where(here, jnp.concatenate([x] * tiles, axis=1), 0.0), axis=0, keepdims=True)

    offsets = spread(fields[0] + 1.0)
    weights = spread(fields[1] + fields[2] + fields[3])
    selector = iota((BINS_DEV, tiles * LANES), 0) + 1 == offsets.astype(jnp.int32)
    chosen = one_hot(selector)
    sums = jnp.dot(chosen[:, :slots], in_ref[...], preferred_element_type=jnp.float32)
    mass = jnp.sum(jnp.where(selector, weights, 0.0), axis=1, keepdims=True) + 1.0
    mean_ref[...] = sums / mass
    lane = (iota(tags.shape, 1) - iota(tags.shape, 0) * stride) & (LANES - 1)
    own = (lane >= capacity) & (lane < capacity + 3)
    total = jnp.sum(jnp.sum(jnp.where(own, tags, 0.0), axis=0, keepdims=True), axis=1, keepdims=True)
    parts = jnp.concatenate([*pieces(weights), jnp.zeros((5, tiles * LANES), jnp.float32)], axis=0)
    over_lanes = (((1,), (1,)), ((), ()))
    masses = lax.dot_general(parts.astype(jnp.bfloat16), chosen, over_lanes, preferred_element_type=jnp.float32)
    masses = jnp.sum(masses, axis=0, keepdims=True) + 1.0
    rarity_ref[...] = jnp.log(total / (BINS_DEV * devices)) - jnp.log(masses)


def shards(goal_embed, goal_bins, goal_weights):
    goals, width = goal_embed.shape
    devices = lax.axis_size("gx") * lax.axis_size("gy")
    capacity = max(2, 2 * goals // devices)
    capacity += capacity % 2
    stride = capacity + 2
    inputs = (goal_embed, goal_bins.reshape(1, goals), goal_weights.reshape(1, goals))
    outgoing = pl.pallas_call(
        lambda *refs: pack(capacity, *refs),
        out_shape=jax.ShapeDtypeStruct((devices * stride, width), jnp.bfloat16),
        in_specs=[pl.BlockSpec(memory_space=pltpu.HBM)] * 3,
        scratch_shapes=[
            pltpu.VMEM((goals, width), goal_embed.dtype),
            pltpu.VMEM((1, goals), goal_bins.dtype),
            pltpu.VMEM((1, goals), goal_weights.dtype),
            pltpu.VMEM((devices * stride, width), jnp.float32),
            pltpu.SemaphoreType.DMA((3,)),
        ],
        compiler_params=pltpu.CompilerParams(vmem_limit_bytes=VMEM_BYTES),
        name="pack",
    )(*(pltpu.with_memory_space_constraint(x, pltpu.HBM) for x in inputs))
    arrived = lax.all_to_all(
        outgoing.reshape(devices, stride // 2, 2, width), ("gy", "gx"), split_axis=0, concat_axis=0, tiled=True
    )
    bin_mean, rarity = pl.pallas_call(
        lambda *refs: unpack(devices, capacity, *refs),
        out_shape=(
            jax.ShapeDtypeStruct((BINS_DEV, width), jnp.float32),
            jax.ShapeDtypeStruct((1, BINS_DEV), jnp.float32),
        ),
        scratch_shapes=[pltpu.VMEM((devices * stride, width), jnp.float32)],
        compiler_params=pltpu.CompilerParams(vmem_limit_bytes=VMEM_BYTES),
        name="unpack",
    )(arrived.reshape(devices * stride, width))
    return bin_mean, rarity.reshape(BINS_DEV)


def solution(mesh):
    in_specs = (P(("gx", "gy"), None), P(("gx", "gy")), P(("gx", "gy")))
    out_specs = (P(("gx", "gy"), None), P(("gx", "gy")))
    return jax.shard_map(shards, mesh=mesh, in_specs=in_specs, out_specs=out_specs, check_vma=False)
```

```python
import jax
import jax.numpy as jnp
from jax import lax
from jax.experimental import pallas as pl
from jax.experimental.pallas import tpu as pltpu
from jax.sharding import PartitionSpec as P

BINS_DEV = 64
LANES = 128
VMEM_BYTES = 4 * 1024 * 1024
FIELD = LANES // 4


def pieces(x):
    hi = x.astype(jnp.bfloat16).astype(jnp.float32)
    rest = x - hi
    mid = rest.astype(jnp.bfloat16).astype(jnp.float32)
    return hi, mid, rest - mid


def one_hot(mask):
    return jnp.where(mask, 1.0, 0.0).astype(jnp.bfloat16)


def quotient(x, n):
    return x >> (n.bit_length() - 1) if n & (n - 1) == 0 else lax.div(x, n)


def iota(shape, dimension):
    return lax.broadcasted_iota(jnp.int32, shape, dimension)


def pack(capacity, embed_hbm, bins_hbm, weights_hbm, out_ref, embed_ref, bins_ref, weights_ref, stage_ref, arrivals):
    goals = embed_ref.shape[0]
    across, along = lax.axis_size("gx"), lax.axis_size("gy")
    devices = across * along
    copies = [
        pltpu.make_async_copy(source, target, arrivals.at[i])
        for i, (source, target) in enumerate(
            ((bins_hbm, bins_ref), (weights_hbm, weights_ref), (embed_hbm, embed_ref))
        )
    ]
    for copy in copies:
        copy.start()
    stride = capacity + 2
    rows = iota((devices * stride, goals), 0)
    for copy in copies[:2]:
        copy.wait()
    bins = bins_ref[...]
    weights = weights_ref[...]
    owners = quotient(bins, BINS_DEV)
    offsets = (bins - owners * BINS_DEV).astype(jnp.float32)
    major = quotient(owners, along)
    owners = (owners - major * along) * across + major
    member = iota((devices, goals), 0) == owners
    earlier = iota((goals, goals), 0) < iota((goals, goals), 1)
    across_rows = jnp.transpose(jnp.broadcast_to(owners.astype(jnp.float32), (goals, goals)))
    before = earlier & (across_rows == owners.astype(jnp.float32))
    places = jnp.sum(jnp.where(before, 1.0, 0.0), axis=0, keepdims=True).astype(jnp.int32)
    chosen = one_hot(rows == owners * stride + places)
    column = jnp.transpose(jnp.broadcast_to(weights, (embed_ref.shape[1], goals)))
    copies[2].wait()
    scaled = (column * embed_ref[...].astype(jnp.float32)).astype(jnp.bfloat16)
    me = lax.axis_index("gy") * across + lax.axis_index("gx")
    tall = pl.cdiv(capacity, 8) * 8
    place = iota((tall, goals), 0) == places
    blank = jnp.zeros((FIELD - tall, goals), jnp.float32)
    tags = []
    for value in (offsets, *pieces(weights)):
        tags += [jnp.where(place, value, 0.0), blank]
    tags = jnp.concatenate(tags, axis=0)
    over_lanes = (((1,), (1,)), ((), ()))
    tags = lax.dot_general(
        one_hot(member), tags.astype(jnp.bfloat16), over_lanes, preferred_element_type=jnp.float32
    )
    lane = iota(tags.shape, 1)
    for i, piece in enumerate(pieces(jnp.sum(weights, axis=1, keepdims=True))):
        tags = jnp.where(lane == capacity + i, piece, tags)
    stage_ref[...] = jnp.dot(chosen, scaled, preferred_element_type=jnp.float32)
    tags = pltpu.roll(tags, (me * stride) & (LANES - 1), 1)
    stage_ref[pl.ds(capacity, devices, stride=stride), :] = tags
    out_ref[...] = stage_ref[...].astype(jnp.bfloat16)


def unpack(devices, capacity, in_ref, mean_ref, rarity_ref, stage_ref):
    stride = capacity + 2
    slots = devices * stride
    stage_ref[...] = in_ref[...].astype(jnp.float32)
    tags = stage_ref[pl.ds(capacity, devices, stride=stride), :]
    fields = [tags, *(pltpu.roll(tags, LANES - field * FIELD, 1) for field in range(1, 4))]
    tiles = pl.cdiv(slots, LANES)
    place = iota((devices, tiles * LANES), 1) - iota((devices, tiles * LANES), 0) * stride
    here = (place >= 0) & (place < capacity)

    def spread(x):
        return jnp.sum(jnp.where(here, jnp.concatenate([x] * tiles, axis=1), 0.0), axis=0, keepdims=True)

    offsets = spread(fields[0] + 1.0)
    weights = spread(fields[1] + fields[2] + fields[3])
    selector = iota((BINS_DEV, tiles * LANES), 0) + 1 == offsets.astype(jnp.int32)
    chosen = one_hot(selector)
    sums = jnp.dot(chosen[:, :slots], in_ref[...], preferred_element_type=jnp.float32)
    mass = jnp.sum(jnp.where(selector, weights, 0.0), axis=1, keepdims=True) + 1.0
    mean_ref[...] = sums / mass
    lane = (iota(tags.shape, 1) - iota(tags.shape, 0) * stride) & (LANES - 1)
    own = (lane >= capacity) & (lane < capacity + 3)
    total = jnp.sum(jnp.sum(jnp.where(own, tags, 0.0), axis=0, keepdims=True), axis=1, keepdims=True)
    parts = jnp.concatenate([*pieces(weights), jnp.zeros((5, tiles * LANES), jnp.float32)], axis=0)
    over_lanes = (((1,), (1,)), ((), ()))
    masses = lax.dot_general(parts.astype(jnp.bfloat16), chosen, over_lanes, preferred_element_type=jnp.float32)
    masses = jnp.sum(masses, axis=0, keepdims=True) + 1.0
    rarity_ref[...] = jnp.log(total / (BINS_DEV * devices)) - jnp.log(masses)


def shards(goal_embed, goal_bins, goal_weights):
    goals, width = goal_embed.shape
    devices = lax.axis_size("gx") * lax.axis_size("gy")
    capacity = max(2, 2 * goals // devices)
    capacity += capacity % 2
    stride = capacity + 2
    inputs = (goal_embed, goal_bins.reshape(1, goals), goal_weights.reshape(1, goals))
    outgoing = pl.pallas_call(
        lambda *refs: pack(capacity, *refs),
        out_shape=jax.ShapeDtypeStruct((devices * stride, width), jnp.bfloat16),
        in_specs=[pl.BlockSpec(memory_space=pltpu.HBM)] * 3,
        scratch_shapes=[
            pltpu.VMEM((goals, width), goal_embed.dtype),
            pltpu.VMEM((1, goals), goal_bins.dtype),
            pltpu.VMEM((1, goals), goal_weights.dtype),
            pltpu.VMEM((devices * stride, width), jnp.float32),
            pltpu.SemaphoreType.DMA((3,)),
        ],
        compiler_params=pltpu.CompilerParams(vmem_limit_bytes=VMEM_BYTES),
        name="pack",
    )(*(pltpu.with_memory_space_constraint(x, pltpu.HBM) for x in inputs))
    arrived = lax.all_to_all(
        outgoing.reshape(devices, stride // 2, 2, width), ("gy", "gx"), split_axis=0, concat_axis=0, tiled=True
    )
    bin_mean, rarity = pl.pallas_call(
        lambda *refs: unpack(devices, capacity, *refs),
        out_shape=(
            jax.ShapeDtypeStruct((BINS_DEV, width), jnp.float32),
            jax.ShapeDtypeStruct((1, BINS_DEV), jnp.float32),
        ),
        scratch_shapes=[pltpu.VMEM((devices * stride, width), jnp.float32)],
        compiler_params=pltpu.CompilerParams(vmem_limit_bytes=VMEM_BYTES),
        name="unpack",
    )(arrived.reshape(devices * stride, width))
    return bin_mean, rarity.reshape(BINS_DEV)


def solution(mesh):
    in_specs = (P(("gx", "gy"), None), P(("gx", "gy")), P(("gx", "gy")))
    out_specs = (P(("gx", "gy"), None), P(("gx", "gy")))
    return jax.shard_map(shards, mesh=mesh, in_specs=in_specs, out_specs=out_specs, check_vma=False)
```
